32 devices in a mesh: dp: 8 (over y, x, core), tensor: 4 (over z).
Axes of the slice: x: 2, y: 2, z: 4, core: 2. Of those that a mesh axis runs over, the one named last changes fastest.
Arguments:
- tokens: bfloat16 [256, 6144], P('dp', 'tensor'), may hold values from -6 to 6
- router_weight: bfloat16 [6144, 8], P('tensor'), may hold values from -0.078125 to 0.078125
- expert_ids: int32 [256, 2], P('dp'), may hold values from 0 to 7, all different within a row; in each aligned block of 32 rows (0 to 31, 32 to 63, ...) at most 12 rows name the same one
- w_gate: bfloat16 [8, 6144, 12288], P('dp', None, 'tensor'), may hold values from -0.078125 to 0.078125
- w_up: bfloat16 [8, 6144, 12288], P('dp', None, 'tensor'), may hold values from -0.078125 to 0.078125
- w_down: bfloat16 [8, 12288, 6144], P('dp', 'tensor'), may hold values from -0.0546875 to 0.0546875
Outputs:
- moe_out: bfloat16 [256, 6144], P('dp', 'tensor')
The draws below stay inside these ranges and needn't reach their ends.
Inputs may be any that keep to these rules, and one draw needn't show every extreme that they name: `expert_ids`: the two experts of a token differ. In each aligned block of 32 rows (the rows of one index of dp) no expert is named by more than 12 rows, a bound that some blocks reach.
All inputs are finite; a program needn't handle non-finite values.
Results may differ from the reference program's by a relative error of at most 0.022.
Values may be sent and summed in bfloat16 or wider, within the bound.
A program may use at most 192 MiB of HBM per device.

```python
import math
import jax
import jax.numpy as jnp
import numpy as np
from jax import lax

D = 6144
FF = 12288
EXPERTS = 8
TOK_DP = 32
CAP = 12
TOKENS = 256
N_DP = 8
N_TENSOR = 4


def block_scale(stream_key, dims, cuts, low, high):
    level, own = 1.0, jax.random.fold_in(stream_key, 6)
    for dim, blocks in cuts:
        draws = jnp.exp(jax.random.uniform(jax.random.fold_in(own, dim), (blocks,), jnp.float32, low / len(cuts), high / len(cuts)))
        level = level * jnp.repeat(draws, dims[dim] // blocks).reshape([-1 if axis == dim else 1 for axis in range(len(dims))])
    return level


def assign_block(rng, own, number, rows, amount, top, bound, slope):
    ranking = jax.random.permutation(rng, amount)
    packed, ordinary = portions_of(amount, rows * top, bound, slope, True), portions_of(amount, rows * top, bound, slope, False)
    places = jnp.arange(amount)

    def named(lengths, offset_by):
        used = int((lengths > 0).sum())
        fixed = max(1, used // 4)
        moved = fixed + (places - fixed + offset_by * (used - fixed)) % max(1, amount - fixed)
        return jnp.zeros((amount,), jnp.int32).at[ranking[jnp.where(places < fixed, places, moved)]].set(jnp.asarray(lengths, jnp.int32))

    lengths = jnp.where(number % 4 == 0, named(packed, number // 4), named(ordinary, number - number // 4 - 1))
    mixed = jax.random.permutation(jax.random.fold_in(own, 3), amount)
    donor, taker = mixed[0:amount // 2 * 2:2], mixed[1:amount // 2 * 2:2]
    slack = jnp.minimum(lengths[donor] - 1, bound - lengths[taker]) // 2
    slack = jnp.where((donor == ranking[0]) | (taker == ranking[0]) | (lengths[taker] == 0), 0, jnp.maximum(slack, 0))
    moved = jax.random.randint(jax.random.fold_in(own, 4), (amount // 2,), 0, 1 << 20) % (slack + 1)
    lengths = lengths.at[donor].add(-moved).at[taker].add(moved)
    labels = jnp.searchsorted(jnp.cumsum(lengths), jnp.arange(rows * top), side="right").astype(jnp.int32)
    grid = labels.reshape(top, rows).T
    grid = grid[jax.random.permutation(jax.random.fold_in(own, 1), rows)]
    offset_by = jax.random.randint(jax.random.fold_in(own, 2), (rows, 1), 0, top)
    return jnp.take_along_axis(grid, (jnp.arange(top)[None, :] + offset_by) % top, axis=1)


def portions_of(number_of, total, most, lean, full):
    portions = [(1 << 20) // math.isqrt(standing ** lean) + 1 for standing in range(1, number_of + 1)]
    largest = most if full else min(most, max(-(-total // number_of), total * portions[0] // sum(portions)))
    least = 1 if total - largest >= number_of - 1 else 0
    given, rest = [largest] + [least] * (number_of - 1), total - largest - least * (number_of - 1)
    while rest > 0:
        candidates = [i for i in range(1, number_of) if given[i] < largest] or [i for i in range(1, number_of) if given[i] < most]
        whole, budget = sum([portions[i] for i in candidates]), rest
        for i in candidates:
            addition = min(most - given[i], max(1, budget * portions[i] // whole), rest)
            given[i] = given[i] + addition
            rest = rest - addition
    return np.array(given)


def gaussian(rng, dims, deviation, reach, split=(), kind=jnp.bfloat16):
    values = deviation * jax.random.normal(rng, dims, jnp.float32)
    if split:
        values = values * block_scale(rng, dims, split, -0.22, 0.18)
    return jnp.clip(values, -reach, reach).astype(kind)


def setup_inputs(seed: int = 0) -> dict:
    key_of = jax.random.split(jax.random.key(seed), 7)
    tokens = gaussian(key_of[0], (TOKENS, D), 1.0, 6.0, ((0, 8), (1, 4)))
    router_weight = gaussian(key_of[1], (D, EXPERTS), D ** -0.5, 0.078125, ((0, 4),))
    expert_ids_keys = jax.random.split(jax.random.fold_in(key_of[2], 1), TOKENS // TOK_DP)
    expert_ids_turns = jax.random.permutation(jax.random.fold_in(key_of[2], 3), TOKENS // TOK_DP)
    expert_ids = jax.vmap(lambda own, number: assign_block(jax.random.fold_in(key_of[2], 2), own, number, TOK_DP, EXPERTS, 2, CAP, 2))(expert_ids_keys, expert_ids_turns).reshape((TOKENS, 2))
    w_gate = gaussian(key_of[3], (N_DP, D, FF // (N_DP // EXPERTS)), D ** -0.5, 0.078125, ((0, 8), (2, 4)))
    w_up = gaussian(key_of[4], (N_DP, D, FF // (N_DP // EXPERTS)), D ** -0.5, 0.078125, ((0, 8), (2, 4)))
    w_down = gaussian(key_of[5], (N_DP, FF // (N_DP // EXPERTS), D), FF ** -0.5, 0.0546875, ((0, 8), (1, 4)))
    return dict(tokens=tokens, router_weight=router_weight, expert_ids=expert_ids, w_gate=w_gate, w_up=w_up, w_down=w_down)


def expert_block(rows, gate_w, up_w, down_w):
    count = rows.shape[0]
    piece = gate_w.shape[2] // N_TENSOR

    def replica(total, parts):
        g_w, u_w, d_w = parts
        gate = jnp.dot(rows, g_w, preferred_element_type=jnp.float32)
        up = jnp.dot(rows, u_w, preferred_element_type=jnp.float32)
        hidden = (jax.nn.silu(gate) * up).astype(jnp.bfloat16)
        hidden_blocks = hidden.reshape(count, N_TENSOR, piece).transpose(1, 0, 2)
        down_blocks = d_w.reshape(N_TENSOR, piece, D)

        def add_block(acc, pair):
            h_part, d_part = pair
            rounded = lax.optimization_barrier(jnp.dot(h_part, d_part, preferred_element_type=jnp.float32).astype(jnp.bfloat16))
            return acc + rounded.astype(jnp.float32), None

        summed, _ = lax.scan(add_block, jnp.zeros((count, D), jnp.float32), (hidden_blocks, down_blocks))
        share = lax.optimization_barrier(summed.astype(jnp.bfloat16))
        return total + share.astype(jnp.float32), None

    result, _ = lax.scan(replica, jnp.zeros((count, D), jnp.float32), (gate_w, up_w, down_w))
    return result


def reference(tokens, router_weight, expert_ids, w_gate, w_up, w_down):
    groups = N_DP // EXPERTS
    slots_all = N_DP * CAP
    logits = jnp.dot(tokens, router_weight, preferred_element_type=jnp.float32)
    chosen = jnp.take_along_axis(logits, expert_ids.astype(jnp.int32), axis=1)
    first = jax.nn.sigmoid(chosen[:, 0] - chosen[:, 1])
    gates = jnp.stack([first, 1.0 - first], axis=1)
    flat = expert_ids.astype(jnp.int32).reshape(N_DP, TOK_DP * 2)
    onehot = (flat[:, :, None] == jnp.arange(EXPERTS, dtype=jnp.int32)[None, None, :]).astype(jnp.int32)
    ranks = jnp.sum((jnp.cumsum(onehot, axis=1).astype(jnp.int32) - onehot) * onehot, axis=2).astype(jnp.int32)
    blocks = jnp.arange(N_DP, dtype=jnp.int32)[:, None]
    position = (flat * slots_all + blocks * CAP + ranks).astype(jnp.int32).reshape(TOKENS, 2)
    buffers = jnp.zeros((EXPERTS * slots_all, D), jnp.bfloat16)
    buffers = buffers.at[position[:, 0]].set(tokens).at[position[:, 1]].set(tokens)
    buffers = buffers.reshape(EXPERTS, slots_all, D)
    gate_all = w_gate.reshape(EXPERTS, groups, D, -1)
    up_all = w_up.reshape(EXPERTS, groups, D, -1)
    down_all = w_down.reshape(EXPERTS, groups, -1, D)
    outputs = lax.map(lambda parts: expert_block(parts[0], parts[1], parts[2], parts[3]), (buffers, gate_all, up_all, down_all))
    outputs = outputs.reshape(EXPERTS * slots_all, D)
    mixed = gates[:, 0:1] * outputs[position[:, 0]] + gates[:, 1:2] * outputs[position[:, 1]]
    return mixed.astype(jnp.bfloat16)
```

```python
import functools

import jax
import jax.numpy as jnp
from jax import lax
from jax.experimental import pallas as pl
from jax.experimental.pallas import tpu as pltpu
from jax.sharding import PartitionSpec as P

EXPERTS = 8
PAD = 16
PIECES = ((0, 8), (8, 4))
LAG = 5
SLOTS = 15
FIRST = 2
AHEAD = 3
LANES = 128
F32 = jnp.float32
BF16 = jnp.bfloat16


def body(dp, nt, n, cb, slots, tok_hbm, rw_hbm, ids_hbm, wg_ref, wu_ref, wd_ref, out_ref,
         wbuf, rows, packed, acc, hidden, ret_out, ret_in, ztok, zout, zin, own, lg_out, lg_in,
         hits, wmat, tokv, rwv, idsv,
         in_sem, w_sem, zt_send, zt_recv, lg_send, lg_recv, d_send, d_recv, r_send, r_recv,
         zo_send, zo_recv):
    me = lax.axis_index("dp")
    t = lax.axis_index("tensor")
    toks, share = tokv.shape
    _, ff = wg_ref.shape
    width = dp * PAD
    groups = dp // EXPERTS
    chunks = ff // n
    kb = min(ff, share)
    kbs = ff // kb
    sub = share // (2 * cb)
    steps = nt * sub
    first_units = nt * chunks
    units = first_units + steps
    mesh = pl.DeviceIdType.MESH

    def order(i):
        near = jnp.where(i % 2 == 1, t - (i + 1) // 2, t + (i + 1) // 2)
        far = jnp.where(t < nt - 1 - t, i, nt - 1 - i)
        return jnp.where(i <= 2 * jnp.minimum(t, nt - 1 - t), near, far)

    def column(s):
        return order(nt - 1 - s // sub), s % sub

    def load(u, act):
        slot = lax.rem(u, slots)

        @pl.when(u < first_units)
        def _():
            deep = pl.ds(pl.multiple_of(order(u // chunks) * share, share), share)
            cols = pl.ds(pl.multiple_of(lax.rem(u, chunks) * n, n), n)
            act(pltpu.make_async_copy(wg_ref.at[deep, cols], wbuf.at[slot, 0], w_sem.at[slot]))
            act(pltpu.make_async_copy(wu_ref.at[deep, cols], wbuf.at[slot, 1], w_sem.at[slots + slot]))

        @pl.when((u >= first_units) & (u < units))
        def _():
            q, j = column(u - first_units)
            for h in range(2):
                for b in range(kbs):
                    cols = pl.ds(pl.multiple_of(q * share + (2 * j + h) * cb, cb), cb)
                    act(pltpu.make_async_copy(
                        wd_ref.at[pl.ds(b * kb, kb), cols],
                        wbuf.at[slot, h, pl.ds(0, kb), pl.ds(b * cb, cb)],
                        w_sem.at[(b * 2 + h) * slots + slot]))

    small = [pltpu.make_async_copy(a, b, in_sem.at[k]) for k, (a, b) in enumerate(
        ((tok_hbm, tokv), (ids_hbm, idsv), (rw_hbm, rwv)))]
    for c in small:
        c.start()

    @pl.loop(0, min(FIRST, units))
    def _(u):
        load(u, lambda c: c.start())

    rows[:, :, 8:PAD, :] = jnp.zeros((nt, dp, PAD - 8, share), BF16)
    ret_in[:, :, 8:PAD, :] = jnp.zeros((steps, dp, PAD - 8, 2 * cb), BF16)
    barrier = pltpu.get_barrier_semaphore()

    @pl.loop(1, dp)
    def _(i):
        pl.semaphore_signal(barrier, inc=1, device_id={"dp": lax.rem(me + i, dp)}, device_id_type=mesh)

    @pl.loop(1, nt)
    def _(i):
        pl.semaphore_signal(barrier, inc=1, device_id={"tensor": lax.rem(t + i, nt)}, device_id_type=mesh)

    @pl.loop(min(FIRST, units), min(slots, units))
    def _(u):
        load(u, lambda c: c.start())

    small[1].wait()
    ids = idsv[...]
    line = lax.broadcasted_iota(jnp.int32, (width, toks), 0)
    expert = line // (PAD * groups)
    rank = (line % PAD).astype(F32)
    named = [ids[k:k + 1, :] == expert for k in range(2)]
    counts = (named[0] | named[1]).astype(F32).astype(BF16)
    upper = (lax.broadcasted_iota(jnp.int32, (toks, toks), 0)
             < lax.broadcasted_iota(jnp.int32, (toks, toks), 1)).astype(F32).astype(BF16)
    before = jnp.dot(counts, upper, preferred_element_type=F32)
    at_rank = before == rank
    for k in range(2):
        hits[k] = (named[k] & at_rank).astype(F32)
    placing = ((named[0] | named[1]) & at_rank).astype(F32).astype(BF16)
    small[0].wait()
    small[2].wait()

    pl.semaphore_wait(barrier, dp + nt - 2)

    @pl.loop(1, nt)
    def _(i):
        pltpu.make_async_remote_copy(
            tokv, ztok.at[t], zt_send.at[i], zt_recv.at[t],
            device_id={"tensor": order(i)}, device_id_type=mesh).start()

    def dispatch(src, value):
        block = jnp.dot(placing, value, preferred_element_type=F32).astype(BF16)
        packed[src] = block.reshape(dp, PAD, share)
        rows[src, me] = packed[src, me]

        @pl.loop(1, dp)
        def _(i):
            p = lax.rem(me + i, dp)
            for k, (a, b) in enumerate(PIECES):
                pltpu.make_async_remote_copy(
                    packed.at[src, p, pl.ds(a, b)], rows.at[src, me, pl.ds(a, b)],
                    d_send.at[src, k], d_recv.at[src, k],
                    device_id={"dp": p}, device_id_type=mesh).start()

    def relay(i):
        src = order(i)
        pltpu.make_async_copy(ztok.at[src], ztok.at[src], zt_recv.at[src]).wait()
        dispatch(src, ztok[src])

    dispatch(t, tokv[...])
    lg_out[...] = jnp.zeros_like(lg_out)
    lg_out[:, 0:toks] = lax.dot_general(rwv[...], tokv[...], (((1,), (1,)), ((), ())),
                                        preferred_element_type=F32)
    lg_in[t] = lg_out[...]

    @pl.loop(1, nt)
    def _(i):
        pltpu.make_async_remote_copy(
            lg_out, lg_in.at[t], lg_send.at[i], lg_recv.at[t],
            device_id={"tensor": order(i)}, device_id_type=mesh).start()

    acc[...] = jnp.zeros_like(acc)

    @pl.loop(1, min(AHEAD, nt))
    def _(i):
        relay(i)

    def products(i, c):
        u = i * chunks + c
        slot = lax.rem(u, slots)
        for k in range(2):
            pltpu.make_async_copy(wbuf.at[slot, k], wbuf.at[slot, k], w_sem.at[k * slots + slot]).wait()
        src = order(i)
        lhs = rows[src].reshape(width, share)
        cols = pl.ds(pl.multiple_of(c * n, n), n)
        out = [acc[k, :, cols] + jnp.dot(lhs, wbuf[slot, k], preferred_element_type=F32)
               for k in range(2)]
        return u, cols, out

    def arrived(i):
        src = order(i)
        for k, (a, b) in enumerate(PIECES):
            view = rows.at[src, pl.ds(0, dp - 1), pl.ds(a, b)]
            pltpu.make_async_copy(view, view, d_recv.at[src, k]).wait()

    @pl.loop(0, nt - 1)
    def _(i):
        arrived(i)

        @pl.loop(0, chunks)
        def _(c):
            u, cols, out = products(i, c)
            for k in range(2):
                acc[k, :, cols] = out[k]
            load(u + slots, lambda d: d.start())

        @pl.when(i + AHEAD < nt)
        def _():
            relay(i + AHEAD)

    arrived(nt - 1)

    @pl.loop(0, chunks)
    def _(c):
        u, cols, (gate, up) = products(nt - 1, c)
        hidden[:, cols] = (gate / (1.0 + jnp.exp(-gate)) * up).astype(BF16)
        load(u + slots, lambda d: d.start())

    @pl.loop(1, nt)
    def _(i):
        src = order(i)
        pltpu.make_async_copy(lg_in.at[src], lg_in.at[src], lg_recv.at[src]).wait()

    logits = jnp.sum(lg_in[...], axis=0)[:, 0:toks]
    which = lax.broadcasted_iota(jnp.int32, logits.shape, 0)
    chosen = [jnp.sum(jnp.where(which == idsv[k:k + 1, :], logits, 0.0), axis=0, keepdims=True)
              for k in range(2)]
    first = jax.nn.sigmoid(chosen[0] - chosen[1])
    w = hits[0] * first + hits[1] * (1.0 - first)
    eye = (lax.broadcasted_iota(jnp.int32, (toks, toks), 0)
           == lax.broadcasted_iota(jnp.int32, (toks, toks), 1)).astype(F32).astype(BF16)
    for k in range(3):
        part = w.astype(BF16)
        wmat[k] = lax.dot_general(eye, part, (((1,), (1,)), ((), ())),
                                  preferred_element_type=F32).astype(BF16)
        w = w - part.astype(F32)

    @pl.loop(0, steps + LAG)
    def _(s):
        @pl.when(s < steps)
        def _():
            u = first_units + s
            slot = lax.rem(u, slots)
            load(u, lambda d: d.wait())
            for h in range(2):
                term = sum(jnp.dot(hidden[:, b * kb:(b + 1) * kb],
                                   wbuf[slot, h, 0:kb, b * cb:(b + 1) * cb],
                                   preferred_element_type=F32) for b in range(kbs))
                ret_out[s, :, :, pl.ds(h * cb, cb)] = term.astype(BF16).reshape(dp, PAD, cb)
            load(u + slots, lambda d: d.start())
            ret_in[s, me] = ret_out[s, me]

            @pl.loop(1, dp)
            def _(i):
                p = lax.rem(me + i, dp)
                for k, (a, b) in enumerate(PIECES):
                    pltpu.make_async_remote_copy(
                        ret_out.at[s, p, pl.ds(a, b)], ret_in.at[s, me, pl.ds(a, b)],
                        r_send.at[s, k], r_recv.at[s, k],
                        device_id={"dp": p}, device_id_type=mesh).start()

        @pl.when(s >= LAG)
        def _():
            b = s - LAG
            q, j = column(b)
            for k, (a, d) in enumerate(PIECES):
                view = ret_in.at[b, pl.ds(0, dp - 1), pl.ds(a, d)]
                pltpu.make_async_copy(view, view, r_recv.at[b, k]).wait()
            back = ret_in[b].reshape(width, 2 * cb)
            mixed = jnp.dot(wmat[0], back, preferred_element_type=F32)
            for k in range(1, 3):
                mixed += jnp.dot(wmat[k], back, preferred_element_type=F32)

            @pl.when(b < steps - sub)
            def _():
                zout[b] = mixed.astype(BF16)
                pltpu.make_async_remote_copy(
                    zout.at[b], zin.at[t, j], zo_send.at[b], zo_recv.at[t * sub + j],
                    device_id={"tensor": q}, device_id_type=mesh).start()

            @pl.when(b >= steps - sub)
            def _():
                own[j] = mixed

    @pl.loop(1, nt)
    def _(i):
        src = lax.rem(t + i, nt)

        @pl.loop(0, sub)
        def _(j):
            pltpu.make_async_copy(zin.at[src, j], zin.at[src, j], zo_recv.at[src * sub + j]).wait()
            own[j] += zin[src, j].astype(F32)

    for j in range(sub):
        out_ref[:, j * 2 * cb:(j + 1) * 2 * cb] = own[j].astype(BF16)

    @pl.loop(1, nt)
    def _(i):
        pltpu.make_async_copy(tokv, tokv, zt_send.at[i]).wait()
        pltpu.make_async_copy(lg_out, lg_out, lg_send.at[i]).wait()

    @pl.loop(0, nt)
    def _(src):
        for k, (a, d) in enumerate(PIECES):
            view = packed.at[src, pl.ds(0, dp - 1), pl.ds(a, d)]
            pltpu.make_async_copy(view, view, d_send.at[src, k]).wait()

    @pl.loop(0, steps)
    def _(s):
        for k, (a, d) in enumerate(PIECES):
            view = ret_out.at[s, pl.ds(0, dp - 1), pl.ds(a, d)]
            pltpu.make_async_copy(view, view, r_send.at[s, k]).wait()

    @pl.loop(0, steps - sub)
    def _(s):
        pltpu.make_async_copy(zout.at[s], zout.at[s], zo_send.at[s]).wait()


def per_device(dp, nt, tokens, router_weight, expert_ids, w_gate, w_up, w_down):
    toks, share = tokens.shape
    _, depth, ff = w_gate.shape
    n = min(512, ff)
    cb = n // (ff // min(ff, share))
    sub = share // (2 * cb)
    steps = nt * sub
    width = dp * PAD
    lanes = -(-toks // LANES) * LANES
    slots = SLOTS
    dma = pltpu.SemaphoreType.DMA
    vm = pl.BlockSpec(memory_space=pltpu.VMEM)
    hbm = pl.BlockSpec(memory_space=pltpu.HBM)
    return pl.pallas_call(
        functools.partial(body, dp, nt, n, cb, slots),
        out_shape=jax.ShapeDtypeStruct((toks, share), BF16),
        in_specs=[hbm] * 6,
        out_specs=vm,
        scratch_shapes=[
            pltpu.VMEM((slots, 2, share, n), BF16),
            pltpu.VMEM((nt, dp, PAD, share), BF16),
            pltpu.VMEM((nt, dp, PAD, share), BF16),
            pltpu.VMEM((2, width, ff), F32),
            pltpu.VMEM((width, ff), BF16),
            pltpu.VMEM((steps, dp, PAD, 2 * cb), BF16),
            pltpu.VMEM((steps, dp, PAD, 2 * cb), BF16),
            pltpu.VMEM((nt, toks, share), BF16),
            pltpu.VMEM((steps, toks, 2 * cb), BF16),
            pltpu.VMEM((nt, sub, toks, 2 * cb), BF16),
            pltpu.VMEM((sub, toks, 2 * cb), F32),
            pltpu.VMEM((EXPERTS, lanes), F32),
            pltpu.VMEM((nt, EXPERTS, lanes), F32),
            pltpu.VMEM((2, width, toks), F32),
            pltpu.VMEM((3, toks, width), BF16),
            pltpu.VMEM((toks, share), BF16),
            pltpu.VMEM((EXPERTS, share), BF16),
            pltpu.VMEM((2, toks), jnp.int32),
            dma((3,)),
            dma((2 * (ff // min(ff, share)) * slots,)),
            dma((nt,)), dma((nt,)), dma((nt,)), dma((nt,)),
            dma((nt, 2)), dma((nt, 2)), dma((steps, 2)), dma((steps, 2)),
            dma((steps,)), dma((steps,)),
        ],
        compiler_params=pltpu.CompilerParams(
            collective_id=0, has_side_effects=True, vmem_limit_bytes=67043328),
    )(tokens, router_weight.T, expert_ids.T, w_gate[0], w_up[0], w_down[0])


def solution(mesh):
    return jax.shard_map(
        functools.partial(per_device, mesh.shape["dp"], mesh.shape["tensor"]),
        mesh=mesh,
        in_specs=(
            P("dp", "tensor"),
            P("tensor", None),
            P("dp", None),
            P("dp", None, "tensor"),
            P("dp", None, "tensor"),
            P("dp", "tensor", None),
        ),
        out_specs=P("dp", "tensor"),
        check_vma=False,
    )
```

```python
import functools

import jax
import jax.numpy as jnp
from jax import lax
from jax.experimental import pallas as pl
from jax.experimental.pallas import tpu as pltpu
from jax.sharding import PartitionSpec as P

EXPERTS = 8
PAD = 16
PIECES = ((0, 8), (8, 4))
LAG = 4
SLOTS = 14
FIRST = 2
AHEAD = 3
UNROLL = 2
LANES = 128
F32 = jnp.float32
BF16 = jnp.bfloat16


def body(dp, nt, n, cb, slots, tok_hbm, rw_hbm, ids_hbm, wg_ref, wu_ref, wd_ref, out_ref,
         wbuf, rows, packed, acc, hidden, ret_in, ztok, zout, zin, own, lg_out, lg_in,
         hits, wmat, tokv, rwv, idsv,
         in_sem, w_sem, own_send, zt_send, zt_recv, lg_send, lg_recv, d_send, d_recv, r_send, r_recv,
         zo_send, zo_recv):
    me = lax.axis_index("dp")
    t = lax.axis_index("tensor")
    toks, share = tokv.shape
    _, ff = wg_ref.shape
    width = dp * PAD
    groups = dp // EXPERTS
    chunks = ff // n
    kb = min(ff, share)
    kbs = ff // kb
    sub = share // (2 * cb)
    steps = nt * sub
    first_units = nt * chunks
    units = first_units + steps
    unroll = max(k for k in range(1, UNROLL + 1) if chunks % k == 0)
    mesh = pl.DeviceIdType.MESH

    def order(i):
        near = jnp.where(i % 2 == 1, t - (i + 1) // 2, t + (i + 1) // 2)
        far = jnp.where(t < nt - 1 - t, i, nt - 1 - i)
        return jnp.where(i <= 2 * jnp.minimum(t, nt - 1 - t), near, far)

    sides = ((t > 0, jnp.maximum(t - 1, 0)), (t < nt - 1, jnp.minimum(t + 1, nt - 1)))
    inner = (t > 0) & (t < nt - 1)
    half = toks // 2

    def column(s):
        return order(nt - 1 - s // sub), s % sub

    def load(u, act):
        slot = lax.rem(u, slots)

        @pl.when(u < first_units)
        def _():
            deep = pl.ds(pl.multiple_of(order(u // chunks) * share, share), share)
            cols = pl.ds(pl.multiple_of(lax.rem(u, chunks) * n, n), n)
            act(pltpu.make_async_copy(wg_ref.at[deep, cols], wbuf.at[slot, 0], w_sem.at[slot]))
            act(pltpu.make_async_copy(wu_ref.at[deep, cols], wbuf.at[slot, 1], w_sem.at[slots + slot]))

        @pl.when((u >= first_units) & (u < units))
        def _():
            q, j = column(u - first_units)
            for h in range(2):
                for b in range(kbs):
                    cols = pl.ds(pl.multiple_of(q * share + (2 * j + h) * cb, cb), cb)
                    act(pltpu.make_async_copy(
                        wd_ref.at[pl.ds(b * kb, kb), cols],
                        wbuf.at[slot, h, pl.ds(0, kb), pl.ds(b * cb, cb)],
                        w_sem.at[(b * 2 + h) * slots + slot]))

    small = [pltpu.make_async_copy(a, b, in_sem.at[k]) for k, (a, b) in enumerate(
        ((tok_hbm, tokv), (ids_hbm, idsv), (rw_hbm, rwv)))]
    for c in small:
        c.start()

    @pl.loop(0, min(FIRST, units))
    def _(u):
        load(u, lambda c: c.start())

    rows[:, :, 8:PAD, :] = jnp.zeros((nt, dp, PAD - 8, share), BF16)
    ret_in[:, :, 8:PAD, :] = jnp.zeros((steps, dp, PAD - 8, 2 * cb), BF16)
    barrier = pltpu.get_barrier_semaphore()

    @pl.loop(1, dp)
    def _(i):
        pl.semaphore_signal(barrier, inc=1, device_id={"dp": lax.rem(me + i, dp)}, device_id_type=mesh)

    for there, beside in sides:
        @pl.when(there)
        def _():
            pl.semaphore_signal(barrier, inc=1, device_id={"tensor": beside}, device_id_type=mesh)

    @pl.loop(min(FIRST, units), min(slots, units))
    def _(u):
        load(u, lambda c: c.start())

    small[1].wait()
    ids = idsv[...]
    line = lax.broadcasted_iota(jnp.int32, (width, toks), 0)
    expert = line // (PAD * groups)
    rank = (line % PAD).astype(F32)
    named = [ids[k:k + 1, :] == expert for k in range(2)]
    counts = (named[0] | named[1]).astype(F32).astype(BF16)
    upper = (lax.broadcasted_iota(jnp.int32, (toks, toks), 0)
             < lax.broadcasted_iota(jnp.int32, (toks, toks), 1)).astype(F32).astype(BF16)
    before = jnp.dot(counts, upper, preferred_element_type=F32)
    at_rank = before == rank
    for k in range(2):
        hits[k] = (named[k] & at_rank).astype(F32)
    placing = ((named[0] | named[1]) & at_rank).astype(F32).astype(BF16)
    small[0].wait()
    small[2].wait()

    pl.semaphore_wait(barrier, dp - 1 + jnp.where(t > 0, 1, 0) + jnp.where(t < nt - 1, 1, 0))

    def piece(ref, h):
        return ref.at[pl.ds(h * half, half)]

    for h in range(2):
        for k, (there, beside) in enumerate(sides):
            @pl.when(there)
            def _():
                pltpu.make_async_remote_copy(
                    piece(tokv, h), piece(ztok.at[t], h), own_send.at[2 * h + k], zt_recv.at[t, h],
                    device_id={"tensor": beside}, device_id_type=mesh).start()

    def dispatch(src, value):
        block = jnp.dot(placing, value, preferred_element_type=F32).astype(BF16)
        packed[src] = block.reshape(dp, PAD, share)
        rows[src, me] = packed[src, me]

        @pl.loop(1, dp)
        def _(i):
            p = lax.rem(me + i, dp)
            for k, (a, b) in enumerate(PIECES):
                pltpu.make_async_remote_copy(
                    packed.at[src, p, pl.ds(a, b)], rows.at[src, me, pl.ds(a, b)],
                    d_send.at[src, k], d_recv.at[src, k],
                    device_id={"dp": p}, device_id_type=mesh).start()

    def forward(i):
        src = order(i)
        for h in range(2):
            block = piece(ztok.at[src], h)
            pltpu.make_async_copy(block, block, zt_recv.at[src, h]).wait()
            for k, (there, beside) in enumerate(sides):
                @pl.when(there & ((src > t) if k == 0 else (src < t)))
                def _():
                    pltpu.make_async_remote_copy(
                        block, block, zt_send.at[src, h], zt_recv.at[src, h],
                        device_id={"tensor": beside}, device_id_type=mesh).start()

    def relay(i):
        forward(i)
        src = order(i)
        dispatch(src, ztok[src])

    dispatch(t, tokv[...])
    lg_out[...] = jnp.zeros_like(lg_out)
    lg_out[:, 0:toks] = lax.dot_general(rwv[...], tokv[...], (((1,), (1,)), ((), ())),
                                        preferred_element_type=F32)
    lg_in[t] = lg_out[...]

    acc[...] = jnp.zeros_like(acc)

    ahead = jnp.where(inner, AHEAD + 1, AHEAD)

    @pl.loop(1, min(AHEAD + 1, nt))
    def _(i):
        @pl.when(i < ahead)
        def _():
            relay(i)

    def products(i, g, finish):
        src = order(i)
        first = i * chunks + g * unroll
        slot = [lax.rem(first + j, slots) for j in range(unroll)]
        for j in range(unroll):
            for k in range(2):
                pltpu.make_async_copy(wbuf.at[slot[j], k], wbuf.at[slot[j], k],
                                      w_sem.at[k * slots + slot[j]]).wait()
        lhs = rows[src].reshape(width, share)
        for j in range(unroll):
            cols = pl.ds(pl.multiple_of((g * unroll + j) * n, n), n)
            finish(cols, [acc[k, :, cols] + jnp.dot(lhs, wbuf[slot[j], k], preferred_element_type=F32)
                          for k in range(2)])
        for j in range(unroll):
            load(first + j + slots, lambda d: d.start())

    def keep(cols, out):
        for k in range(2):
            acc[k, :, cols] = out[k]

    def activate(cols, out):
        gate, up = out
        hidden[:, cols] = (gate / (1.0 + jnp.exp(-gate)) * up).astype(BF16)

    def arrived(i):
        src = order(i)
        for k, (a, b) in enumerate(PIECES):
            view = rows.at[src, pl.ds(0, dp - 1), pl.ds(a, b)]
            pltpu.make_async_copy(view, view, d_recv.at[src, k]).wait()

    @pl.loop(0, nt - 1)
    def _(i):
        arrived(i)

        @pl.loop(0, chunks // unroll)
        def _(g):
            products(i, g, keep)

        @pl.when(i + ahead < nt)
        def _():
            relay(i + ahead)

    @pl.loop(1, nt)
    def _(i):
        pltpu.make_async_remote_copy(
            lg_out, lg_in.at[t], lg_send.at[i], lg_recv.at[t],
            device_id={"tensor": order(i)}, device_id_type=mesh).start()

    arrived(nt - 1)

    @pl.loop(0, chunks // unroll)
    def _(g):
        products(nt - 1, g, activate)

    @pl.loop(0, nt)
    def _(src):
        for k, (a, d) in enumerate(PIECES):
            view = packed.at[src, pl.ds(0, dp - 1), pl.ds(a, d)]
            pltpu.make_async_copy(view, view, d_send.at[src, k]).wait()

    def gating():
        @pl.loop(1, nt)
        def _(i):
            src = order(i)
            pltpu.make_async_copy(lg_in.at[src], lg_in.at[src], lg_recv.at[src]).wait()

        logits = jnp.sum(lg_in[...], axis=0)[:, 0:toks]
        which = lax.broadcasted_iota(jnp.int32, logits.shape, 0)
        chosen = [jnp.sum(jnp.where(which == idsv[k:k + 1, :], logits, 0.0), axis=0, keepdims=True)
                  for k in range(2)]
        first = jax.nn.sigmoid(chosen[0] - chosen[1])
        w = hits[0] * first + hits[1] * (1.0 - first)
        eye = (lax.broadcasted_iota(jnp.int32, (toks, toks), 0)
               == lax.broadcasted_iota(jnp.int32, (toks, toks), 1)).astype(F32).astype(BF16)
        for k in range(3):
            part = w.astype(BF16)
            wmat[k] = lax.dot_general(eye, part, (((1,), (1,)), ((), ())),
                                      preferred_element_type=F32).astype(BF16)
            w = w - part.astype(F32)

    @pl.loop(0, steps + LAG)
    def _(s):
        @pl.when(s < steps)
        def _():
            u = first_units + s
            slot = lax.rem(u, slots)
            load(u, lambda d: d.wait())
            for h in range(2):
                term = sum(jnp.dot(hidden[:, b * kb:(b + 1) * kb],
                                   wbuf[slot, h, 0:kb, b * cb:(b + 1) * cb],
                                   preferred_element_type=F32) for b in range(kbs))
                packed[s // sub, :, :, pl.ds(pl.multiple_of((s % sub) * 2 * cb + h * cb, cb), cb)] = (
                    term.astype(BF16).reshape(dp, PAD, cb))
            load(u + slots, lambda d: d.start())
            cols = pl.ds(pl.multiple_of((s % sub) * 2 * cb, 2 * cb), 2 * cb)
            ret_in[s, me] = packed[s // sub, me, :, cols]

            @pl.loop(1, dp)
            def _(i):
                p = lax.rem(me + i, dp)
                for k, (a, b) in enumerate(PIECES):
                    pltpu.make_async_remote_copy(
                        packed.at[s // sub, p, pl.ds(a, b), cols], ret_in.at[s, me, pl.ds(a, b)],
                        r_send.at[s, k], r_recv.at[s, k],
                        device_id={"dp": p}, device_id_type=mesh).start()

        @pl.when(s == LAG)
        def _():
            gating()

        @pl.when(s >= LAG)
        def _():
            b = s - LAG
            q, j = column(b)
            for k, (a, d) in enumerate(PIECES):
                view = ret_in.at[b, pl.ds(0, dp - 1), pl.ds(a, d)]
                pltpu.make_async_copy(view, view, r_recv.at[b, k]).wait()
            back = ret_in[b].reshape(width, 2 * cb)
            mixed = jnp.dot(wmat[0], back, preferred_element_type=F32)
            for k in range(1, 3):
                mixed += jnp.dot(wmat[k], back, preferred_element_type=F32)

            @pl.when(b < steps - sub)
            def _():
                zout[b] = mixed.astype(BF16)
                pltpu.make_async_remote_copy(
                    zout.at[b], zin.at[t, j], zo_send.at[b], zo_recv.at[t * sub + j],
                    device_id={"tensor": q}, device_id_type=mesh).start()

            @pl.when(b >= steps - sub)
            def _():
                own[j] = mixed

    @pl.loop(1, nt)
    def _(i):
        src = lax.rem(t + i, nt)

        @pl.loop(0, sub)
        def _(j):
            pltpu.make_async_copy(zin.at[src, j], zin.at[src, j], zo_recv.at[src * sub + j]).wait()
            own[j] += zin[src, j].astype(F32)

    for j in range(sub):
        out_ref[:, j * 2 * cb:(j + 1) * 2 * cb] = own[j].astype(BF16)

    for h in range(2):
        for k, (there, beside) in enumerate(sides):
            @pl.when(there)
            def _():
                pltpu.make_async_copy(piece(tokv, h), piece(tokv, h), own_send.at[2 * h + k]).wait()

            @pl.loop(0, nt)
            def _(src):
                @pl.when(there & ((src > t) if k == 0 else (src < t)))
                def _():
                    block = piece(ztok.at[src], h)
                    pltpu.make_async_copy(block, block, zt_send.at[src, h]).wait()

    @pl.loop(1, nt)
    def _(i):
        pltpu.make_async_copy(lg_out, lg_out, lg_send.at[i]).wait()

    @pl.loop(0, steps)
    def _(s):
        for k, (a, d) in enumerate(PIECES):
            view = ret_in.at[s, pl.ds(0, dp - 1), pl.ds(a, d)]
            pltpu.make_async_copy(view, view, r_send.at[s, k]).wait()

    @pl.loop(0, steps - sub)
    def _(s):
        pltpu.make_async_copy(zout.at[s], zout.at[s], zo_send.at[s]).wait()


def per_device(dp, nt, tokens, router_weight, expert_ids, w_gate, w_up, w_down):
    toks, share = tokens.shape
    _, depth, ff = w_gate.shape
    n = min(512, ff)
    cb = n // (ff // min(ff, share))
    sub = share // (2 * cb)
    steps = nt * sub
    width = dp * PAD
    lanes = -(-toks // LANES) * LANES
    slots = SLOTS
    dma = pltpu.SemaphoreType.DMA
    vm = pl.BlockSpec(memory_space=pltpu.VMEM)
    hbm = pl.BlockSpec(memory_space=pltpu.HBM)
    return pl.pallas_call(
        functools.partial(body, dp, nt, n, cb, slots),
        out_shape=jax.ShapeDtypeStruct((toks, share), BF16),
        in_specs=[hbm] * 6,
        out_specs=vm,
        scratch_shapes=[
            pltpu.VMEM((slots, 2, share, n), BF16),
            pltpu.VMEM((nt, dp, PAD, share), BF16),
            pltpu.VMEM((nt, dp, PAD, share), BF16),
            pltpu.VMEM((2, width, ff), F32),
            pltpu.VMEM((width, ff), BF16),
            pltpu.VMEM((steps, dp, PAD, 2 * cb), BF16),
            pltpu.VMEM((nt, toks, share), BF16),
            pltpu.VMEM((steps, toks, 2 * cb), BF16),
            pltpu.VMEM((nt, sub, toks, 2 * cb), BF16),
            pltpu.VMEM((sub, toks, 2 * cb), F32),
            pltpu.VMEM((EXPERTS, lanes), F32),
            pltpu.VMEM((nt, EXPERTS, lanes), F32),
            pltpu.VMEM((2, width, toks), F32),
            pltpu.VMEM((3, toks, width), BF16),
            pltpu.VMEM((toks, share), BF16),
            pltpu.VMEM((EXPERTS, share), BF16),
            pltpu.VMEM((2, toks), jnp.int32),
            dma((3,)),
            dma((2 * (ff // min(ff, share)) * slots,)),
            dma((4,)), dma((nt, 2)), dma((nt, 2)), dma((nt,)), dma((nt,)),
            dma((nt, 2)), dma((nt, 2)), dma((steps, 2)), dma((steps, 2)),
            dma((steps,)), dma((steps,)),
        ],
        compiler_params=pltpu.CompilerParams(
            collective_id=0, has_side_effects=True, vmem_limit_bytes=55836672),
    )(*[pltpu.with_memory_space_constraint(x, pltpu.HBM) for x in (tokens, router_weight.T, expert_ids.T)], w_gate[0], w_up[0], w_down[0])


def solution(mesh):
    return jax.shard_map(
        functools.partial(per_device, mesh.shape["dp"], mesh.shape["tensor"]),
        mesh=mesh,
        in_specs=(
            P("dp", "tensor"),
            P("tensor", None),
            P("dp", None),
            P("dp", None, "tensor"),
            P("dp", None, "tensor"),
            P("dp", "tensor", None),
        ),
        out_specs=P("dp", "tensor"),
        check_vma=False,
    )
```
